256 devices in a mesh: seq: 2 (over core), ctx: 32 (over x, z_hi, y), tp: 4 (over z_lo).
Axes of the slice: x: 4, y: 4, z: 8 (z_hi: 2, z_lo: 4; z = z_hi * 4 + z_lo), core: 2. Of those that a mesh axis runs over, the one named last changes fastest.
Arguments:
- queries: bfloat16 [16384, 16, 128], P(('seq', 'ctx'), 'tp'), parts along dimension 0, may hold values from -160 to 160
- key_rows: bfloat16 [16384, 4, 128], P(('seq', 'ctx'), 'tp'), parts along dimension 0, may hold values from -5 to 5
- value_slot_rows: bfloat16 [16384, 4, 128], P(('seq', 'ctx'), 'tp'), parts along dimension 0, may hold values from -6 to 6
- out_grad: bfloat16 [16384, 16, 128], P(('seq', 'ctx'), 'tp'), parts along dimension 0, may hold values from -6 to 6
- span_order: int32 [128], P('seq'), parts along dimension 0, may hold values from 0 to 63, each once
Outputs:
- query_grad: bfloat16 [16384, 16, 128], P(('seq', 'ctx'), 'tp'), parts along dimension 0
- key_gradient: bfloat16 [16384, 4, 128], P(('seq', 'ctx'), 'tp'), parts along dimension 0
- value_gradient: bfloat16 [16384, 4, 128], P(('seq', 'ctx'), 'tp'), parts along dimension 0
The draws below stay inside these ranges and needn't reach their ends.
There are 2 independent parts, one for each index of `seq`. The reference program is written for one: setup_inputs(seed, part) draws one part's arguments, and reference() takes and returns one part's arrays. A program takes and returns all parts, laid end to end along the dimension named above; each array names one. Nothing has to cross between parts.
Inputs may be any that keep to these rules, and one draw needn't show every extreme that they name: Slot s of 128 rows holds span span_order[s] of the sequence; every span number stands once.
All inputs are finite; a program needn't handle non-finite values.
Results may differ from the reference program's by a relative error of at most 0.0085.
Values may be sent and summed in bfloat16 or wider, within the bound.
No kernel may reach another device: no remote copies, remote signals or barrier semaphores. Data moves between devices by JAX's collectives and lax.ppermute only.
A program may use at most 64 MiB of HBM per device.

```python
import math
import jax
import jax.numpy as jnp
from jax import lax

HEAD_SIZE = 128
QUERY_HEADS = 16
KEY_VALUE_HEADS = 4
SPAN = 128
SLOTS = 64
SEQUENCE_TOKENS = 8192


def keys_base(key):
    return jax.random.truncated_normal(jax.random.fold_in(key, 7), -5.0, 5.0, (SEQUENCE_TOKENS, KEY_VALUE_HEADS, HEAD_SIZE), jnp.float32)


def draw_key_rows(key, part):
    values = keys_base(key)
    return values.astype(jnp.bfloat16)


def draw_queries(key, part):
    values = jax.random.truncated_normal(jax.random.fold_in(key, 11), -5.0, 5.0, (SEQUENCE_TOKENS, QUERY_HEADS, HEAD_SIZE), jnp.float32)
    return values.astype(jnp.bfloat16)


def steps_of(key, extent, cuts, smallest, top_value):
    def one(position, shards_of):
        draws = jax.random.uniform(jax.random.fold_in(jax.random.fold_in(key, 6), position), (shards_of,), jnp.float32, smallest / len(cuts), top_value / len(cuts))
        return jnp.repeat(jnp.exp(draws), extent[position] // shards_of).reshape((-1,) + (1,) * (len(extent) - position - 1))

    loudness = one(*cuts[0])
    for cut in cuts[1:]:
        loudness = loudness * one(*cut)
    return loudness


def scatter_about(key, dims, spread, bound, pieces=(), held_as=jnp.bfloat16):
    result = spread * jax.random.normal(key, dims, jnp.float32)
    if pieces:
        result = result * steps_of(key, dims, pieces, -0.22, 0.18)
    return jnp.clip(result, -bound, bound).astype(held_as)


def setup_inputs(seed: int = 0, part: int = 0) -> dict:
    key_list = jax.random.split(jax.random.key(seed), 6)
    own_keys = jax.random.split(jax.random.fold_in(key_list[5], part), 6)
    return {
        "queries": draw_queries(jax.random.fold_in(jax.random.fold_in(key_list[5], part), 71), part),
        "key_rows": draw_key_rows(jax.random.fold_in(jax.random.fold_in(key_list[5], part), 71), part),
        "value_slot_rows": scatter_about(own_keys[2], (SEQUENCE_TOKENS, KEY_VALUE_HEADS, HEAD_SIZE), 1.0, 6.0, ((0, 32), (1, 4))),
        "out_grad": scatter_about(own_keys[3], (SEQUENCE_TOKENS, QUERY_HEADS, HEAD_SIZE), 1.0, 6.0, ((0, 32), (1, 4))),
        "span_order": jax.random.permutation(own_keys[4], SLOTS).astype(jnp.int32),
    }


NEGATIVE = -1e+30

def positions_of(span_order):
    offsets = jnp.tile(jnp.arange(SPAN, dtype=jnp.int32), SLOTS)
    return (jnp.repeat(span_order.astype(jnp.int32), SPAN) * SPAN + offsets).astype(jnp.int32)

def head_grads(query_head, key_head, value_head, grad_head, places):
    scaling = 1.0 / math.sqrt(HEAD_SIZE)
    value_wide = value_head.astype(jnp.float32)

    def step(carried, block_index):
        key_acc, value_acc = carried
        begin = (block_index * SPAN).astype(jnp.int32)
        q_block = lax.dynamic_slice_in_dim(query_head, begin, SPAN, 0)
        g_block = lax.dynamic_slice_in_dim(grad_head, begin, SPAN, 0)
        q_places = lax.dynamic_slice_in_dim(places, begin, SPAN, 0)
        visible = q_places[:, None] >= places[None, :]
        scores = jnp.dot(q_block, key_head.T, preferred_element_type=jnp.float32) * scaling
        scores = jnp.where(visible, scores, NEGATIVE)
        row_top = lax.optimization_barrier(jnp.max(scores, axis=1, keepdims=True))
        row_sum = lax.optimization_barrier(jnp.sum(jnp.where(visible, jnp.exp(scores - row_top), 0.0), axis=1, keepdims=True))
        log_total = row_top + jnp.log(row_sum)
        probs = jnp.where(visible, jnp.exp(scores - log_total), 0.0)
        probs_low = probs.astype(jnp.bfloat16)
        output = jnp.dot(probs, value_wide, precision=lax.Precision.HIGHEST, preferred_element_type=jnp.float32)
        row_delta = lax.optimization_barrier(jnp.sum(g_block.astype(jnp.float32) * output, axis=1, keepdims=True))
        grad_probs = jnp.dot(g_block, value_head.T, preferred_element_type=jnp.float32)
        grad_scores = (probs * (grad_probs - row_delta) * scaling).astype(jnp.bfloat16)
        query_part = jnp.dot(grad_scores, key_head, preferred_element_type=jnp.float32).astype(jnp.bfloat16)
        key_acc = key_acc + jnp.dot(grad_scores.T, q_block, preferred_element_type=jnp.float32)
        value_acc = value_acc + jnp.dot(probs_low.T, g_block, preferred_element_type=jnp.float32)
        return ((key_acc, value_acc), query_part)
    zeros = jnp.zeros((SEQUENCE_TOKENS, HEAD_SIZE), jnp.float32)
    (key_acc, value_acc), query_parts = lax.scan(step, (zeros, zeros), jnp.arange(SEQUENCE_TOKENS // SPAN, dtype=jnp.int32))
    return (query_parts.reshape(SEQUENCE_TOKENS, HEAD_SIZE), key_acc, value_acc)

def reference(queries, key_rows, value_slot_rows, out_grad, span_order):
    places = positions_of(span_order)
    query_cluster = QUERY_HEADS // KEY_VALUE_HEADS

    def per_head(head):
        kv_head = head // query_cluster
        query_head = lax.dynamic_index_in_dim(queries, head, 1, keepdims=False)
        grad_head = lax.dynamic_index_in_dim(out_grad, head, 1, keepdims=False)
        key_head = lax.dynamic_index_in_dim(key_rows, kv_head, 1, keepdims=False)
        value_head = lax.dynamic_index_in_dim(value_slot_rows, kv_head, 1, keepdims=False)
        return head_grads(query_head, key_head, value_head, grad_head, places)
    query_all, key_complete, value_complete = lax.map(per_head, jnp.arange(QUERY_HEADS, dtype=jnp.int32))
    query_grad = jnp.transpose(query_all, (1, 0, 2))
    key_gradient = jnp.transpose(key_complete.reshape(KEY_VALUE_HEADS, query_cluster, SEQUENCE_TOKENS, HEAD_SIZE).sum(axis=1), (1, 0, 2)).astype(jnp.bfloat16)
    value_gradient = jnp.transpose(value_complete.reshape(KEY_VALUE_HEADS, query_cluster, SEQUENCE_TOKENS, HEAD_SIZE).sum(axis=1), (1, 0, 2)).astype(jnp.bfloat16)
    return (query_grad, key_gradient, value_gradient)
```

```python
import math

import jax
import jax.numpy as jnp
from jax import lax
from jax.experimental import pallas as pl
from jax.experimental.pallas import tpu as pltpu
from jax.sharding import PartitionSpec as P

NEG = -1e30
X, Z, Y = 4, 2, 4
SPAN = 128
D = 128
HEADS = 4
ROWS = HEADS * SPAN
LOCAL = 2
RS = X * LOCAL
KS = Y * Z * LOCAL
SCALE = 1.0 / math.sqrt(D)
C2 = SCALE * math.log2(math.e)


def ctx_index(x, z, y):
    return (x * Z + z) * Y + y


def shift(dx=0, dz=0, dy=0):
    return [
        (ctx_index((x + dx) % X, (z + dz) % Z, (y + dy) % Y), ctx_index(x, z, y))
        for x in range(X)
        for z in range(Z)
        for y in range(Y)
    ]


def fetch(a, **d):
    return lax.ppermute(a, "ctx", shift(**d))


def plan(order_ref, pos_ref, rank_ref, kspan_ref, rspan_ref):
    x, z, y = pos_ref[0], pos_ref[1], pos_ref[2]
    for s in range(X):
        for e in range(LOCAL):
            dev = ((x + s) % X * Z + z) * Y + y
            rspan_ref[s * LOCAL + e] = order_ref[dev * LOCAL + e]
    ks = []
    for w in range(Z):
        for t in range(Y):
            dev = (x * Z + (z + w) % Z) * Y + (y + t) % Y
            for e in range(LOCAL):
                k = order_ref[dev * LOCAL + e]
                kspan_ref[(w * Y + t) * LOCAL + e] = k
                ks.append(k)
    for i in range(KS):
        r = jnp.int32(0)
        for j in range(KS):
            if j != i:
                r = r + (ks[j] < ks[i]).astype(jnp.int32)
        rank_ref[r] = i


def counts(kspan_ref, p):
    below = jnp.int32(0)
    upto = jnp.int32(0)
    for i in range(KS):
        k = kspan_ref[i]
        below = below + (k < p).astype(jnp.int32)
        upto = upto + (k <= p).astype(jnp.int32)
    return below // 2, upto - below // 2 * 2


def pair_of(ref, a, b):
    return jnp.concatenate([ref[a], ref[b]], axis=0)


def nt(a, b):
    return lax.dot_general(a, b, (((1,), (1,)), ((), ())), preferred_element_type=jnp.float32)


def nn(a, b):
    return lax.dot_general(a, b, (((1,), (0,)), ((), ())), preferred_element_type=jnp.float32)


def hide(st, kspan_ref, a, b, p):
    key = lax.broadcasted_iota(jnp.int32, (SPAN, ROWS), 0)
    row = lax.broadcasted_iota(jnp.int32, (SPAN, ROWS), 1) % SPAN
    ahead = key - row
    sa = jnp.where(ahead <= (p - kspan_ref[a]) * SPAN, st[:SPAN], NEG)
    sb = jnp.where(ahead <= (p - kspan_ref[b]) * SPAN, st[SPAN:], NEG)
    return jnp.concatenate([sa, sb], axis=0)


def stats_kernel(order_ref, pos_ref, *refs):
    qg = refs[:X]
    kv = refs[X : X + Y * Z]
    out_ref = refs[X + Y * Z]
    qs, gs, ks, vs, rank_ref, kspan_ref, rspan_ref = refs[X + Y * Z + 1 :]
    plan(order_ref, pos_ref, rank_ref, kspan_ref, rspan_ref)
    for s in range(X):
        for e in range(LOCAL):
            qs[s * LOCAL + e] = qg[s][e, 0]
            gs[s * LOCAL + e] = qg[s][e, 1]
    for i in range(Y * Z):
        for e in range(LOCAL):
            ks[i * LOCAL + e] = kv[i][0, e]
            vs[i * LOCAL + e] = kv[i][1, e]

    @pl.loop(0, RS)
    def _(r):
        p = rspan_ref[r]
        full, rest = counts(kspan_ref, p)

        def tile(j, carried, masked):
            m, l, d = carried
            a, b = rank_ref[2 * j], rank_ref[2 * j + 1]
            st = nt(pair_of(ks, a, b), qs[r])
            dp = nt(pair_of(vs, a, b), gs[r])
            if masked:
                st = hide(st, kspan_ref, a, b, p)
            top = jnp.maximum(m, jnp.max(st, axis=0, keepdims=True))
            keep = jnp.exp2((m - top) * C2)
            e = jnp.exp2((st - top) * C2)
            l = l * keep + jnp.sum(e, axis=0, keepdims=True)
            d = d * keep + jnp.sum(e * dp, axis=0, keepdims=True)
            return top, l, d

        def put(carried):
            for i in range(3):
                for h in range(HEADS):
                    out_ref[r // 2, i, pl.ds(r % 2 * HEADS + h, 1), :] = carried[i][:, h * SPAN : (h + 1) * SPAN]

        start = (
            jnp.full((1, ROWS), NEG, jnp.float32),
            jnp.zeros((1, ROWS), jnp.float32),
            jnp.zeros((1, ROWS), jnp.float32),
        )
        state = lax.fori_loop(0, full, lambda j, c: tile(j, c, False), start)
        put(state)

        @pl.when(rest > 0)
        def _():
            put(tile(full, state, True))


def grads_kernel(order_ref, pos_ref, *refs):
    qg = refs[:X]
    kv = refs[X : X + Y * Z]
    st_refs = refs[X + Y * Z : 2 * X + Y * Z]
    n = 2 * X + Y * Z
    dq_refs = refs[n : n + X]
    dkv_ref = refs[n + X]
    qs, gs, ks, vs, kt, lse_ref, delta_ref, dqt, dk, dv, rank_ref, kspan_ref, rspan_ref = refs[n + X + 1 :]
    plan(order_ref, pos_ref, rank_ref, kspan_ref, rspan_ref)
    for s in range(X):
        for e in range(LOCAL):
            qs[s * LOCAL + e] = qg[s][e, 0]
            gs[s * LOCAL + e] = qg[s][e, 1]
    for i in range(Y * Z):
        for e in range(LOCAL):
            k = kv[i][0, e]
            ks[i * LOCAL + e] = k
            vs[i * LOCAL + e] = kv[i][1, e]
            kt[i * LOCAL + e] = k.T
    for s in range(X):
        parts = [st_refs[t][(s - t) % X] for t in range(X)]
        top = parts[0][0]
        for q in parts[1:]:
            top = jnp.maximum(top, q[0])
        total = jnp.zeros_like(top)
        dots = jnp.zeros_like(top)
        for q in parts:
            f = jnp.exp2((q[0] - top) * C2)
            total = total + q[1] * f
            dots = dots + q[2] * f
        lse_ref[pl.ds(s * 8, 8), :] = top * C2 + jnp.log2(total)
        delta_ref[pl.ds(s * 8, 8), :] = dots / total
    dk[...] = jnp.zeros_like(dk)
    dv[...] = jnp.zeros_like(dv)

    @pl.loop(0, RS)
    def _(r):
        p = rspan_ref[r]
        full, rest = counts(kspan_ref, p)
        lse = jnp.concatenate([lse_ref[pl.ds(r * HEADS + h, 1), :] for h in range(HEADS)], axis=1)
        delta = jnp.concatenate([delta_ref[pl.ds(r * HEADS + h, 1), :] for h in range(HEADS)], axis=1)
        dqt[...] = jnp.zeros_like(dqt)

        def tile(j, masked):
            a, b = rank_ref[2 * j], rank_ref[2 * j + 1]
            q, g = qs[r], gs[r]
            st = nt(pair_of(ks, a, b), q)
            dp = nt(pair_of(vs, a, b), g)
            if masked:
                st = hide(st, kspan_ref, a, b, p)
            pt = jnp.exp2(st * C2 - lse)
            ds = (pt * (dp - delta)).astype(jnp.bfloat16)
            dvt = nn(pt.astype(jnp.bfloat16), g)
            dkt = nn(ds, q)
            dv[a] += dvt[:SPAN]
            dv[b] += dvt[SPAN:]
            dk[a] += dkt[:SPAN]
            dk[b] += dkt[SPAN:]
            dqt[...] += nn(jnp.concatenate([kt[a], kt[b]], axis=1), ds)

        @pl.loop(0, full)
        def _(j):
            tile(j, False)

        @pl.when(rest > 0)
        def _():
            tile(full, True)

        for s in range(X):
            @pl.when(r // 2 == s)
            def _():
                dq_refs[s][r % 2] = (dqt[...] * SCALE).T.astype(jnp.bfloat16)

    for i in range(Y * Z):
        for e in range(LOCAL):
            dkv_ref[i, 0, e] = (dk[i * LOCAL + e] * SCALE).astype(jnp.bfloat16)
            dkv_ref[i, 1, e] = dv[i * LOCAL + e].astype(jnp.bfloat16)


SMEM = pl.BlockSpec(memory_space=pltpu.SMEM)
VMEM = pl.BlockSpec(memory_space=pltpu.VMEM)


def index_scratch():
    return [pltpu.SMEM((KS,), jnp.int32), pltpu.SMEM((KS,), jnp.int32), pltpu.SMEM((RS,), jnp.int32)]


def operand_scratch():
    return [
        pltpu.VMEM((RS, ROWS, D), jnp.bfloat16),
        pltpu.VMEM((RS, ROWS, D), jnp.bfloat16),
        pltpu.VMEM((KS, SPAN, D), jnp.bfloat16),
        pltpu.VMEM((KS, SPAN, D), jnp.bfloat16),
    ]


def stats_call(order, pos, qg, kv):
    return pl.pallas_call(
        stats_kernel,
        out_shape=jax.ShapeDtypeStruct((X, 3, LOCAL * HEADS, SPAN), jnp.float32),
        in_specs=[SMEM, SMEM] + [VMEM] * (len(qg) + len(kv)),
        out_specs=VMEM,
        scratch_shapes=operand_scratch() + index_scratch(),
        compiler_params=pltpu.CompilerParams(vmem_limit_bytes=48 * 2**20),
        name="row_stats",
    )(order, pos, *qg, *kv)


def grads_call(order, pos, qg, kv, stats):
    return pl.pallas_call(
        grads_kernel,
        out_shape=[jax.ShapeDtypeStruct((LOCAL, ROWS, D), jnp.bfloat16)] * X
        + [jax.ShapeDtypeStruct((Y * Z, 2, LOCAL, SPAN, D), jnp.bfloat16)],
        in_specs=[SMEM, SMEM] + [VMEM] * (len(qg) + len(kv) + len(stats)),
        out_specs=[VMEM] * (X + 1),
        scratch_shapes=operand_scratch()
        + [
            pltpu.VMEM((KS, D, SPAN), jnp.bfloat16),
            pltpu.VMEM((RS * HEADS, SPAN), jnp.float32),
            pltpu.VMEM((RS * HEADS, SPAN), jnp.float32),
            pltpu.VMEM((D, ROWS), jnp.float32),
            pltpu.VMEM((KS, SPAN, D), jnp.float32),
            pltpu.VMEM((KS, SPAN, D), jnp.float32),
        ]
        + index_scratch(),
        compiler_params=pltpu.CompilerParams(vmem_limit_bytes=48 * 2**20),
        name="gradients",
    )(order, pos, *qg, *kv, *stats)


def by_head(a):
    return a.reshape(LOCAL, SPAN, HEADS, D).transpose(0, 2, 1, 3).reshape(LOCAL, ROWS, D)


def local(queries, key_rows, value_slot_rows, out_grad, span_order):
    me = lax.axis_index("ctx")
    pos = jnp.stack([me // (Z * Y), me // Y % Z, me % Y]).astype(jnp.int32)
    kv0 = jnp.stack([key_rows.reshape(LOCAL, SPAN, D), value_slot_rows.reshape(LOCAL, SPAN, D)])
    qg0 = jnp.stack([by_head(queries), by_head(out_grad)], axis=1)
    kvz = fetch(kv0, dz=1)
    qg = [qg0] + [fetch(qg0, dx=s) for s in range(1, X)]
    kv = [kv0] + [fetch(kv0, dy=t) for t in range(1, Y)] + [kvz] + [fetch(kvz, dy=t) for t in range(1, Y)]
    stats0 = stats_call(span_order, pos, qg, kv)
    stats = [stats0] + [fetch(stats0, dx=t) for t in range(1, X)]
    *dq, dkv = grads_call(span_order, pos, qg, kv, stats)

    other = dkv[Y].astype(jnp.float32)
    for t in range(1, Y):
        other = other + fetch(dkv[Y + t], dy=-t).astype(jnp.float32)
    own = dkv[0].astype(jnp.float32)
    for t in range(1, Y):
        own = own + fetch(dkv[t], dy=-t).astype(jnp.float32)
    own = own + fetch(other.astype(jnp.bfloat16), dz=1).astype(jnp.float32)
    own = own.astype(jnp.bfloat16)
    key_gradient = own[0].reshape(LOCAL * SPAN, 1, D)
    value_gradient = own[1].reshape(LOCAL * SPAN, 1, D)
    total = dq[0].astype(jnp.float32)
    for s in range(1, X):
        total = total + fetch(dq[s], dx=-s).astype(jnp.float32)
    query_grad = (
        total.astype(jnp.bfloat16)
        .reshape(LOCAL, HEADS, SPAN, D)
        .transpose(0, 2, 1, 3)
        .reshape(LOCAL * SPAN, HEADS, D)
    )
    return query_grad, key_gradient, value_gradient


def solution(mesh):
    spec = P(("seq", "ctx"), "tp", None)
    return jax.shard_map(
        local,
        mesh=mesh,
        in_specs=(spec, spec, spec, spec, P("seq")),
        out_specs=(spec, spec, spec),
        check_vma=False,
    )
```

```python
import math

import jax
import jax.numpy as jnp
from jax import lax
from jax.experimental import pallas as pl
from jax.experimental.pallas import tpu as pltpu
from jax.sharding import PartitionSpec as P


NEG = -1e30
X, Z, Y = 4, 2, 4
SPAN = 128
D = 128
HEADS = 4
ROWS = HEADS * SPAN
LOCAL = 2
LINE = (0, 1, 3, 2)
NEAR = LINE[:-1]
PLANE = tuple((w, t) for w in range(Z) for t in range(Y))
HALF = Y * LOCAL
SCALE = 1.0 / math.sqrt(D)
C2 = SCALE * math.log2(math.e)
UNROLL = 2
COST = 1
FAR = 60.0


def ctx_index(x, z, y):
    return (x * Z + z) * Y + y


def shift(dx=0, dz=0, dy=0):
    return [
        (ctx_index((x + dx) % X, (z + dz) % Z, (y + dy) % Y), ctx_index(x, z, y))
        for x in range(X)
        for z in range(Z)
        for y in range(Y)
    ]


def fetch(a, **d):
    return lax.ppermute(a, "ctx", shift(**d))


def plan(rows, keys, group, order_ref, pos_ref, rank_ref, kspan_ref, rspan_ref):
    x, z, y = pos_ref[0], pos_ref[1], pos_ref[2]
    for i, s in enumerate(rows):
        dev = ((x + s) % X * Z + z) * Y + y
        for e in range(LOCAL):
            rspan_ref[i * LOCAL + e] = order_ref[dev * LOCAL + e]
    ks = []
    for w, t in keys:
        dev = (x * Z + (z + w) % Z) * Y + (y + t) % Y
        for e in range(LOCAL):
            k = order_ref[dev * LOCAL + e]
            kspan_ref[len(ks)] = k
            ks.append(k)
    for i in range(len(ks)):
        base = i // group * group
        r = jnp.int32(base)
        for j in range(base, base + group):
            if j != i:
                r = r + (ks[j] < ks[i]).astype(jnp.int32)
        rank_ref[r] = i


def pairs_upto(kspan_ref, base, n, p):
    upto = jnp.int32(1)
    for i in range(n):
        upto = upto + (kspan_ref[base + i] <= p).astype(jnp.int32)
    return upto // 2


def take(qg, kv, qs, gs, ks, vs):
    spans = [(ref, e) for ref in qg for e in range(ref.shape[0])]
    for i, (ref, e) in enumerate(spans):
        qs[i] = ref[e, 0]
        gs[i] = ref[e, 1]
    for i, ref in enumerate(kv):
        for e in range(LOCAL):
            ks[i * LOCAL + e] = ref[0, e]
            vs[i * LOCAL + e] = ref[1, e]


def pair_of(ref, a, b):
    return jnp.concatenate([ref[a], ref[b]], axis=0)


def nt(a, b):
    return lax.dot_general(a, b, (((1,), (1,)), ((), ())), preferred_element_type=jnp.float32)


def nn(a, b):
    return lax.dot_general(a, b, (((1,), (0,)), ((), ())), preferred_element_type=jnp.float32)


def hide(st, kspan_ref, a, b, p):
    key = lax.broadcasted_iota(jnp.int32, (SPAN, ROWS), 0)
    row = lax.broadcasted_iota(jnp.int32, (SPAN, ROWS), 1) % SPAN
    ahead = key - row
    sa = jnp.where(ahead <= (p - kspan_ref[a]) * SPAN, st[:SPAN], NEG)
    sb = jnp.where(ahead <= (p - kspan_ref[b]) * SPAN, st[SPAN:], NEG)
    return jnp.concatenate([sa, sb], axis=0)


def below(x):
    return jnp.sum(x, axis=0, keepdims=True)


def stats_kernel(rows, keys, order_ref, pos_ref, *refs):
    nq, nk = len(rows), len(keys)
    first = nk == Y
    n = nq if first else nq + 1
    qg = refs[:n]
    kv = refs[n : n + nk]
    refs = refs[n + nk :]
    if not first:
        init_ref, refs = refs[0], refs[1:]
    out_ref, qs, gs, ks, vs, over_ref, rank_ref, kspan_ref, rspan_ref = refs
    plan(rows, keys, HALF, order_ref, pos_ref, rank_ref, kspan_ref, rspan_ref)
    take(qg, kv, qs, gs, ks, vs)
    over_ref[...] = jnp.zeros_like(over_ref)

    def begin():
        for i in range(nq):
            if not first and i < len(NEAR):
                out_ref[i] = init_ref[i]
            else:
                out_ref[i, 0] = jnp.full((LOCAL * HEADS, SPAN), NEG, jnp.float32)
                out_ref[i, 1] = jnp.zeros((LOCAL * HEADS, SPAN), jnp.float32)
                out_ref[i, 2] = jnp.zeros((LOCAL * HEADS, SPAN), jnp.float32)

    if first:
        jobs = nq * LOCAL
    else:
        jobs = (nq - len(NEAR)) * LOCAL + nq * LOCAL

    def work(job, careful):
        if first:
            r, base = job, 0
        else:
            early = job < jobs - nq * LOCAL
            r = jnp.where(early, job + len(NEAR) * LOCAL, job - (jobs - nq * LOCAL))
            base = jnp.where(early, 0, HALF)
        p = rspan_ref[r]
        pairs = pairs_upto(kspan_ref, base, HALF, p)

        def get():
            return tuple(
                jnp.concatenate(
                    [out_ref[r // 2, i, pl.ds(r % 2 * HEADS + h, 1), :] for h in range(HEADS)], axis=1
                )
                for i in range(3)
            )

        def put(carried):
            for i in range(3):
                for h in range(HEADS):
                    out_ref[r // 2, i, pl.ds(r % 2 * HEADS + h, 1), :] = carried[i][:, h * SPAN : (h + 1) * SPAN]

        def products(j):
            a, b = rank_ref[base + 2 * j], rank_ref[base + 2 * j + 1]
            return nt(pair_of(ks, a, b), qs[r]), nt(pair_of(vs, a, b), gs[r]), a, b

        def exact(j, carried):
            m, l, d = carried
            st, dp, a, b = products(j)
            st = hide(st, kspan_ref, a, b, p)
            top = jnp.maximum(m, jnp.max(st, axis=0, keepdims=True))
            keep = jnp.exp2((m - top) * C2)
            e = jnp.exp2((st - top) * C2)
            return top, l * keep + below(e), d * keep + below(e * dp)

        def quick(j, n, ref, carried):
            m, l, d = carried
            for i in range(n):
                st, dp, _, _ = products(j + i)
                m = jnp.maximum(m, jnp.max(st, axis=0, keepdims=True))
                e = jnp.exp2(st * C2 - ref)
                l = l + below(e)
                d = d + below(e * dp)
            return m, l, d

        if careful:
            put(lax.fori_loop(0, pairs, exact, get()))
            return

        @pl.when(pairs > 0)
        def _():
            m, l, d = exact(pairs - 1, get())
            rest = pairs - 1
            many = rest // UNROLL
            ref = m * C2
            state = lax.fori_loop(0, many, lambda j, c: quick(j * UNROLL, UNROLL, ref, c), (m, l, d))
            top, l, d = lax.fori_loop(many * UNROLL, rest, lambda j, c: quick(j, 1, ref, c), state)
            put((m, l, d))
            over_ref[...] = jnp.maximum(over_ref[...], top - m)

    begin()

    @pl.loop(0, jobs)
    def _(job):
        work(job, False)

    @pl.when(jnp.max(over_ref[...]) * C2 > FAR)
    def _():
        begin()

        @pl.loop(0, jobs)
        def _(job):
            work(job, True)


def grads_kernel(order_ref, pos_ref, *refs):
    qg = refs[: X + 1]
    kv = refs[X + 1 : X + 1 + Y * Z]
    n = X + 1 + Y * Z
    st_refs = refs[n : n + X]
    n = n + X
    dq_refs = refs[n : n + X]
    dkv_refs = refs[n + X : n + X + Y * Z]
    qs, gs, ks, vs, kt, lse_ref, delta_ref, dqt, dk, dv, rank_ref, kspan_ref, rspan_ref = refs[n + X + Y * Z :]
    nk = Y * Z * LOCAL
    plan(LINE, PLANE, nk, order_ref, pos_ref, rank_ref, kspan_ref, rspan_ref)
    take(qg, kv, qs, gs, ks, vs)
    for i in range(nk):
        kt[i] = ks[i].T
    for i, s in enumerate(LINE):
        parts = [st_refs[t][LINE.index((s - t) % X)] for t in range(X)]
        top = parts[0][0]
        for q in parts[1:]:
            top = jnp.maximum(top, q[0])
        total = jnp.zeros_like(top)
        dots = jnp.zeros_like(top)
        for q in parts:
            f = jnp.exp2((q[0] - top) * C2)
            total = total + q[1] * f
            dots = dots + q[2] * f
        lse_ref[pl.ds(i * 8, 8), :] = top * C2 + jnp.log2(total)
        delta_ref[pl.ds(i * 8, 8), :] = dots / total
    dk[...] = jnp.zeros_like(dk)
    dv[...] = jnp.zeros_like(dv)

    @pl.loop(0, X * LOCAL)
    def _(r):
        p = rspan_ref[r]
        pairs = pairs_upto(kspan_ref, 0, nk, p)
        lse = jnp.concatenate([lse_ref[pl.ds(r * HEADS + h, 1), :] for h in range(HEADS)], axis=1)
        delta = jnp.concatenate([delta_ref[pl.ds(r * HEADS + h, 1), :] for h in range(HEADS)], axis=1)

        def tile(j, n, masked):
            q, g = qs[r], gs[r]
            to_q = None
            for i in range(n):
                a, b = rank_ref[2 * (j + i)], rank_ref[2 * (j + i) + 1]
                st = nt(pair_of(ks, a, b), q)
                dp = nt(pair_of(vs, a, b), g)
                if masked:
                    st = hide(st, kspan_ref, a, b, p)
                pt = jnp.exp2(st * C2 - lse)
                ds = (pt * (dp - delta)).astype(jnp.bfloat16)
                dvt = nn(pt.astype(jnp.bfloat16), g)
                dkt = nn(ds, q)
                dv[a] += dvt[:SPAN]
                dv[b] += dvt[SPAN:]
                dk[a] += dkt[:SPAN]
                dk[b] += dkt[SPAN:]
                part = nn(jnp.concatenate([kt[a], kt[b]], axis=1), ds)
                to_q = part if to_q is None else to_q + part
            if masked:
                dqt[r] = to_q
            else:
                dqt[r] += to_q

        @pl.when(pairs == 0)
        def _():
            dqt[r] = jnp.zeros((D, ROWS), jnp.float32)

        @pl.when(pairs > 0)
        def _():
            tile(pairs - 1, 1, True)
            many = (pairs - 1) // UNROLL

            @pl.loop(0, many)
            def _(j):
                tile(j * UNROLL, UNROLL, False)

            @pl.loop(many * UNROLL, pairs - 1)
            def _(j):
                tile(j, 1, False)

    for i in range(X):
        for e in range(LOCAL):
            dq_refs[i][e] = (dqt[i * LOCAL + e] * SCALE).T.astype(jnp.bfloat16)
    for i in range(Y * Z):
        for e in range(LOCAL):
            dkv_refs[i][0, e] = (dk[i * LOCAL + e] * SCALE).astype(jnp.bfloat16)
            dkv_refs[i][1, e] = dv[i * LOCAL + e].astype(jnp.bfloat16)


SMEM = pl.BlockSpec(memory_space=pltpu.SMEM)
VMEM = pl.BlockSpec(memory_space=pltpu.VMEM)


def index_scratch(nq, nk):
    return [
        pltpu.SMEM((nk * LOCAL,), jnp.int32),
        pltpu.SMEM((nk * LOCAL,), jnp.int32),
        pltpu.SMEM((nq * LOCAL,), jnp.int32),
    ]


def operand_scratch(nq, nk):
    return [
        pltpu.VMEM((nq * LOCAL, ROWS, D), jnp.bfloat16),
        pltpu.VMEM((nq * LOCAL, ROWS, D), jnp.bfloat16),
        pltpu.VMEM((nk * LOCAL, SPAN, D), jnp.bfloat16),
        pltpu.VMEM((nk * LOCAL, SPAN, D), jnp.bfloat16),
    ]


def cost(nq, nk, products):
    return pl.CostEstimate(
        flops=nq * nk * LOCAL * ROWS * LOCAL * SPAN * D * 2 * products * COST,
        bytes_accessed=(nq * 4 * ROWS + nk * 4 * SPAN) * D * 2,
        transcendentals=0,
    )


def stats_call(order, pos, qg, kv, rows, keys, *init):
    nq, nk = len(rows), len(keys)
    return pl.pallas_call(
        lambda *refs: stats_kernel(rows, keys, *refs),
        out_shape=jax.ShapeDtypeStruct((nq, 3, LOCAL * HEADS, SPAN), jnp.float32),
        in_specs=[SMEM, SMEM] + [VMEM] * (len(qg) + nk + len(init)),
        out_specs=VMEM,
        scratch_shapes=operand_scratch(nq, nk) + [pltpu.VMEM((1, ROWS), jnp.float32)] + index_scratch(nq, nk),
        compiler_params=pltpu.CompilerParams(vmem_limit_bytes=48 * 2**20),
        cost_estimate=cost(nq, nk, 2),
        name="row_stats",
    )(order, pos, *qg, *kv, *init)


def grads_call(order, pos, qg, kv, stats):
    nk = Y * Z * LOCAL
    return pl.pallas_call(
        grads_kernel,
        out_shape=[jax.ShapeDtypeStruct((LOCAL, ROWS, D), jnp.bfloat16)] * X
        + [jax.ShapeDtypeStruct((2, LOCAL, SPAN, D), jnp.bfloat16)] * (Y * Z),
        in_specs=[SMEM, SMEM] + [VMEM] * (len(qg) + len(kv) + len(stats)),
        out_specs=[VMEM] * (X + Y * Z),
        scratch_shapes=operand_scratch(X, Y * Z)
        + [
            pltpu.VMEM((nk, D, SPAN), jnp.bfloat16),
            pltpu.VMEM((X * LOCAL * HEADS, SPAN), jnp.float32),
            pltpu.VMEM((X * LOCAL * HEADS, SPAN), jnp.float32),
            pltpu.VMEM((X * LOCAL, D, ROWS), jnp.float32),
            pltpu.VMEM((nk, SPAN, D), jnp.float32),
            pltpu.VMEM((nk, SPAN, D), jnp.float32),
        ]
        + index_scratch(X, Y * Z),
        compiler_params=pltpu.CompilerParams(vmem_limit_bytes=48 * 2**20),
        cost_estimate=cost(X, Y * Z, 5),
        name="gradients",
    )(order, pos, *qg, *kv, *stats)


def by_head(a):
    return a.reshape(LOCAL, SPAN, HEADS, D).transpose(0, 2, 1, 3).reshape(LOCAL, ROWS, D)


def step(queries, key_rows, value_slot_rows, out_grad, span_order):
    me = lax.axis_index("ctx")
    pos = jnp.stack([me // (Z * Y), me // Y % Z, me % Y]).astype(jnp.int32)
    kv0 = jnp.stack([key_rows.reshape(LOCAL, SPAN, D), value_slot_rows.reshape(LOCAL, SPAN, D)])
    qg0 = jnp.stack([by_head(queries), by_head(out_grad)], axis=1)
    kvz = fetch(kv0, dz=1)
    qg = [qg0, fetch(qg0, dx=1), fetch(qg0, dx=3)]
    kv = [kv0] + [fetch(kv0, dy=t) for t in range(1, Y)]
    part = stats_call(span_order, pos, qg, kv, NEAR, PLANE[:Y])
    qg += [fetch(qg[1][:1], dx=1), fetch(qg[2][1:], dx=3)]
    kv += [kvz] + [fetch(kvz, dy=t) for t in range(1, Y)]
    stats0 = stats_call(span_order, pos, qg, kv, LINE, PLANE, part)
    stats = [stats0] + [fetch(stats0, dx=t) for t in range(1, X)]
    out = grads_call(span_order, pos, qg, kv, stats)
    dq, own, other = out[:X], out[X : X + Y], out[X + Y :]

    def add(parts):
        total = parts[0].astype(jnp.float32)
        for p in parts[1:]:
            total = total + p.astype(jnp.float32)
        return total

    other = add([other[0]] + [fetch(other[t], dy=-t) for t in range(1, Y)]).astype(jnp.bfloat16)
    other = fetch(other, dz=1)
    own = add([own[0]] + [fetch(own[t], dy=-t) for t in range(1, Y)] + [other]).astype(jnp.bfloat16)
    key_gradient = own[0].reshape(LOCAL * SPAN, 1, D)
    value_gradient = own[1].reshape(LOCAL * SPAN, 1, D)
    total = add([dq[0]] + [fetch(dq[i], dx=-s) for i, s in enumerate(LINE) if i > 0])
    query_grad = (
        total.astype(jnp.bfloat16)
        .reshape(LOCAL, HEADS, SPAN, D)
        .transpose(0, 2, 1, 3)
        .reshape(LOCAL * SPAN, HEADS, D)
    )
    return query_grad, key_gradient, value_gradient


def solution(mesh):
    spec = P(("seq", "ctx"), "tp", None)
    return jax.shard_map(
        step,
        mesh=mesh,
        in_specs=(spec, spec, spec, spec, P("seq")),
        out_specs=(spec, spec, spec),
        check_vma=False,
    )
```

```python
import math

import jax
import jax.numpy as jnp
from jax import lax
from jax.experimental import pallas as pl
from jax.experimental.pallas import tpu as pltpu
from jax.sharding import PartitionSpec as P


NEG = -1e30
X, Z, Y = 4, 2, 4
SPAN = 128
D = 128
HEADS = 4
ROWS = HEADS * SPAN
LOCAL = 2
LINE = (0, 1, 3, 2)
NEAR = LINE[:-1]
PLANE = tuple((w, t) for w in range(Z) for t in range(Y))
HALF = Y * LOCAL
SCALE = 1.0 / math.sqrt(D)
C2 = SCALE * math.log2(math.e)
UNROLL = 2
COST = 1
FAR = 60.0


def ctx_index(x, z, y):
    return (x * Z + z) * Y + y


def shift(dx=0, dz=0, dy=0):
    return [
        (ctx_index((x + dx) % X, (z + dz) % Z, (y + dy) % Y), ctx_index(x, z, y))
        for x in range(X)
        for z in range(Z)
        for y in range(Y)
    ]


def fetch(a, **d):
    return lax.ppermute(a, "ctx", shift(**d))


def plan(rows, keys, group, order_ref, pos_ref, rank_ref, kspan_ref, rspan_ref):
    x, z, y = pos_ref[0], pos_ref[1], pos_ref[2]
    for i, s in enumerate(rows):
        dev = ((x + s) % X * Z + z) * Y + y
        for e in range(LOCAL):
            rspan_ref[i * LOCAL + e] = order_ref[dev * LOCAL + e]
    ks = []
    for w, t in keys:
        dev = (x * Z + (z + w) % Z) * Y + (y + t) % Y
        for e in range(LOCAL):
            k = order_ref[dev * LOCAL + e]
            kspan_ref[len(ks)] = k
            ks.append(k)
    for i in range(len(ks)):
        base = i // group * group
        r = jnp.int32(base)
        for j in range(base, base + group):
            if j != i:
                r = r + (ks[j] < ks[i]).astype(jnp.int32)
        rank_ref[r] = i


def pairs_upto(kspan_ref, base, n, p):
    upto = jnp.int32(1)
    for i in range(n):
        upto = upto + (kspan_ref[base + i] <= p).astype(jnp.int32)
    return upto // 2


def take(qg, kv, qs, gs, ks, vs):
    spans = [(ref, e) for ref in qg for e in range(ref.shape[0])]
    for i, (ref, e) in enumerate(spans):
        qs[i] = ref[e, 0]
        gs[i] = ref[e, 1]
    for i, ref in enumerate(kv):
        for e in range(LOCAL):
            ks[i * LOCAL + e] = ref[0, e]
            vs[i * LOCAL + e] = ref[1, e]


def pair_of(ref, a, b):
    return jnp.concatenate([ref[a], ref[b]], axis=0)


def nt(a, b):
    return lax.dot_general(a, b, (((1,), (1,)), ((), ())), preferred_element_type=jnp.float32)


def nn(a, b):
    return lax.dot_general(a, b, (((1,), (0,)), ((), ())), preferred_element_type=jnp.float32)


def hide(st, kspan_ref, a, b, p):
    key = lax.broadcasted_iota(jnp.int32, (SPAN, ROWS), 0)
    row = lax.broadcasted_iota(jnp.int32, (SPAN, ROWS), 1) % SPAN
    ahead = key - row
    sa = jnp.where(ahead <= (p - kspan_ref[a]) * SPAN, st[:SPAN], NEG)
    sb = jnp.where(ahead <= (p - kspan_ref[b]) * SPAN, st[SPAN:], NEG)
    return jnp.concatenate([sa, sb], axis=0)


def below(x):
    return jnp.sum(x, axis=0, keepdims=True)


def stats_kernel(rows, keys, order_ref, pos_ref, *refs):
    nq, nk = len(rows), len(keys)
    first = nk == Y
    n = nq if first else nq + 1
    qg = refs[:n]
    kv = refs[n : n + nk]
    refs = refs[n + nk :]
    if not first:
        init_ref, refs = refs[0], refs[1:]
    out_ref, qs, gs, ks, vs, over_ref, rank_ref, kspan_ref, rspan_ref = refs
    plan(rows, keys, HALF, order_ref, pos_ref, rank_ref, kspan_ref, rspan_ref)
    take(qg, kv, qs, gs, ks, vs)
    over_ref[...] = jnp.zeros_like(over_ref)

    def begin():
        for i in range(nq):
            if not first and i < len(NEAR):
                out_ref[i] = init_ref[i]
            else:
                out_ref[i, 0] = jnp.full((LOCAL * HEADS, SPAN), NEG, jnp.float32)
                out_ref[i, 1] = jnp.zeros((LOCAL * HEADS, SPAN), jnp.float32)
                out_ref[i, 2] = jnp.zeros((LOCAL * HEADS, SPAN), jnp.float32)

    if first:
        jobs = nq * LOCAL
    else:
        jobs = (nq - len(NEAR)) * LOCAL + nq * LOCAL

    def work(job, careful):
        if first:
            r, base = job, 0
        else:
            early = job < jobs - nq * LOCAL
            r = jnp.where(early, job + len(NEAR) * LOCAL, job - (jobs - nq * LOCAL))
            base = jnp.where(early, 0, HALF)
        p = rspan_ref[r]
        pairs = pairs_upto(kspan_ref, base, HALF, p)

        def get():
            return tuple(
                jnp.concatenate(
                    [out_ref[r // 2, i, pl.ds(r % 2 * HEADS + h, 1), :] for h in range(HEADS)], axis=1
                )
                for i in range(3)
            )

        def put(carried):
            for i in range(3):
                for h in range(HEADS):
                    out_ref[r // 2, i, pl.ds(r % 2 * HEADS + h, 1), :] = carried[i][:, h * SPAN : (h + 1) * SPAN]

        def products(j):
            a, b = rank_ref[base + 2 * j], rank_ref[base + 2 * j + 1]
            return nt(pair_of(ks, a, b), qs[r]), nt(pair_of(vs, a, b), gs[r]), a, b

        def exact(j, carried):
            m, l, d = carried
            st, dp, a, b = products(j)
            st = hide(st, kspan_ref, a, b, p)
            top = jnp.maximum(m, jnp.max(st, axis=0, keepdims=True))
            keep = jnp.exp2((m - top) * C2)
            e = jnp.exp2((st - top) * C2)
            return top, l * keep + below(e), d * keep + below(e * dp)

        def quick(j, n, ref, carried):
            m, l, d = carried
            for i in range(n):
                st, dp, _, _ = products(j + i)
                m = jnp.maximum(m, jnp.max(st, axis=0, keepdims=True))
                e = jnp.exp2(st * C2 - ref)
                l = l + below(e)
                d = d + below(e * dp)
            return m, l, d

        if careful:
            put(lax.fori_loop(0, pairs, exact, get()))
            return

        @pl.when(pairs > 0)
        def _():
            m, l, d = exact(pairs - 1, get())
            rest = pairs - 1
            many = rest // UNROLL
            ref = m * C2
            state = lax.fori_loop(0, many, lambda j, c: quick(j * UNROLL, UNROLL, ref, c), (m, l, d))
            top, l, d = lax.fori_loop(many * UNROLL, rest, lambda j, c: quick(j, 1, ref, c), state)
            put((m, l, d))
            over_ref[...] = jnp.maximum(over_ref[...], top - m)

    begin()

    @pl.loop(0, jobs)
    def _(job):
        work(job, False)

    @pl.when(jnp.max(over_ref[...]) * C2 > FAR)
    def _():
        begin()

        @pl.loop(0, jobs)
        def _(job):
            work(job, True)


def grads_kernel(order_ref, pos_ref, *refs):
    qg = refs[: X + 1]
    kv = refs[X + 1 : X + 1 + Y * Z]
    n = X + 1 + Y * Z
    st_refs = refs[n : n + X]
    n = n + X
    dq_refs = refs[n : n + X]
    dkv_refs = refs[n + X : n + X + Y * Z]
    qs, gs, ks, vs, kt, lse_ref, delta_ref, dqt, dk, dv, rank_ref, kspan_ref, rspan_ref = refs[n + X + Y * Z :]
    nk = Y * Z * LOCAL
    plan(LINE, PLANE, nk, order_ref, pos_ref, rank_ref, kspan_ref, rspan_ref)
    take(qg, kv, qs, gs, ks, vs)
    for i in range(nk):
        kt[i] = ks[i].T
    for i, s in enumerate(LINE):
        parts = [st_refs[t][LINE.index((s - t) % X)] for t in range(X)]
        top = parts[0][0]
        for q in parts[1:]:
            top = jnp.maximum(top, q[0])
        total = jnp.zeros_like(top)
        dots = jnp.zeros_like(top)
        for q in parts:
            f = jnp.exp2((q[0] - top) * C2)
            total = total + q[1] * f
            dots = dots + q[2] * f
        lse_ref[pl.ds(i * 8, 8), :] = top * C2 + jnp.log2(total)
        delta_ref[pl.ds(i * 8, 8), :] = dots / total
    dk[...] = jnp.zeros_like(dk)
    dv[...] = jnp.zeros_like(dv)

    @pl.loop(0, X * LOCAL)
    def _(r):
        p = rspan_ref[r]
        pairs = pairs_upto(kspan_ref, 0, nk, p)
        lse = jnp.concatenate([lse_ref[pl.ds(r * HEADS + h, 1), :] for h in range(HEADS)], axis=1)
        delta = jnp.concatenate([delta_ref[pl.ds(r * HEADS + h, 1), :] for h in range(HEADS)], axis=1)

        def tile(j, n, masked):
            q, g = qs[r], gs[r]
            to_q = None
            for i in range(n):
                a, b = rank_ref[2 * (j + i)], rank_ref[2 * (j + i) + 1]
                st = nt(pair_of(ks, a, b), q)
                dp = nt(pair_of(vs, a, b), g)
                if masked:
                    st = hide(st, kspan_ref, a, b, p)
                pt = jnp.exp2(st * C2 - lse)
                ds = (pt * (dp - delta)).astype(jnp.bfloat16)
                dvt = nn(pt.astype(jnp.bfloat16), g)
                dkt = nn(ds, q)
                dv[a] += dvt[:SPAN]
                dv[b] += dvt[SPAN:]
                dk[a] += dkt[:SPAN]
                dk[b] += dkt[SPAN:]
                part = nn(jnp.concatenate([kt[a], kt[b]], axis=1), ds)
                to_q = part if to_q is None else to_q + part
            if masked:
                dqt[r] = to_q
            else:
                dqt[r] += to_q

        @pl.when(pairs == 0)
        def _():
            dqt[r] = jnp.zeros((D, ROWS), jnp.float32)

        @pl.when(pairs > 0)
        def _():
            tile(pairs - 1, 1, True)
            many = (pairs - 1) // UNROLL

            @pl.loop(0, many)
            def _(j):
                tile(j * UNROLL, UNROLL, False)

            @pl.loop(many * UNROLL, pairs - 1)
            def _(j):
                tile(j, 1, False)

    for i in range(X):
        for e in range(LOCAL):
            dq_refs[i][e] = (dqt[i * LOCAL + e] * SCALE).T.astype(jnp.bfloat16)
    for i in range(Y * Z):
        for e in range(LOCAL):
            dkv_refs[i][0, e] = (dk[i * LOCAL + e] * SCALE).astype(jnp.bfloat16)
            dkv_refs[i][1, e] = dv[i * LOCAL + e].astype(jnp.bfloat16)


SMEM = pl.BlockSpec(memory_space=pltpu.SMEM)
VMEM = pl.BlockSpec(memory_space=pltpu.VMEM)


def index_scratch(nq, nk):
    return [
        pltpu.SMEM((nk * LOCAL,), jnp.int32),
        pltpu.SMEM((nk * LOCAL,), jnp.int32),
        pltpu.SMEM((nq * LOCAL,), jnp.int32),
    ]


def operand_scratch(nq, nk):
    return [
        pltpu.VMEM((nq * LOCAL, ROWS, D), jnp.bfloat16),
        pltpu.VMEM((nq * LOCAL, ROWS, D), jnp.bfloat16),
        pltpu.VMEM((nk * LOCAL, SPAN, D), jnp.bfloat16),
        pltpu.VMEM((nk * LOCAL, SPAN, D), jnp.bfloat16),
    ]


def cost(nq, nk, products):
    return pl.CostEstimate(
        flops=nq * nk * LOCAL * ROWS * LOCAL * SPAN * D * 2 * products * COST,
        bytes_accessed=(nq * 4 * ROWS + nk * 4 * SPAN) * D * 2,
        transcendentals=0,
    )


def stats_call(order, pos, qg, kv, rows, keys, *init):
    nq, nk = len(rows), len(keys)
    return pl.pallas_call(
        lambda *refs: stats_kernel(rows, keys, *refs),
        out_shape=jax.ShapeDtypeStruct((nq, 3, LOCAL * HEADS, SPAN), jnp.float32),
        in_specs=[SMEM, SMEM] + [VMEM] * (len(qg) + nk + len(init)),
        out_specs=VMEM,
        scratch_shapes=operand_scratch(nq, nk) + [pltpu.VMEM((1, ROWS), jnp.float32)] + index_scratch(nq, nk),
        compiler_params=pltpu.CompilerParams(vmem_limit_bytes=48 * 2**20),
        cost_estimate=cost(nq, nk, 2),
        name="row_stats",
    )(order, pos, *qg, *kv, *init)


def grads_call(order, pos, qg, kv, stats):
    nk = Y * Z * LOCAL
    return pl.pallas_call(
        grads_kernel,
        out_shape=[jax.ShapeDtypeStruct((LOCAL, ROWS, D), jnp.bfloat16)] * X
        + [jax.ShapeDtypeStruct((2, LOCAL, SPAN, D), jnp.bfloat16)] * (Y * Z),
        in_specs=[SMEM, SMEM] + [VMEM] * (len(qg) + len(kv) + len(stats)),
        out_specs=[VMEM] * (X + Y * Z),
        scratch_shapes=operand_scratch(X, Y * Z)
        + [
            pltpu.VMEM((nk, D, SPAN), jnp.bfloat16),
            pltpu.VMEM((X * LOCAL * HEADS, SPAN), jnp.float32),
            pltpu.VMEM((X * LOCAL * HEADS, SPAN), jnp.float32),
            pltpu.VMEM((X * LOCAL, D, ROWS), jnp.float32),
            pltpu.VMEM((nk, SPAN, D), jnp.float32),
            pltpu.VMEM((nk, SPAN, D), jnp.float32),
        ]
        + index_scratch(X, Y * Z),
        compiler_params=pltpu.CompilerParams(vmem_limit_bytes=48 * 2**20),
        cost_estimate=cost(X, Y * Z, 5),
        name="gradients",
    )(order, pos, *qg, *kv, *stats)


def by_head(a):
    return a.reshape(LOCAL, SPAN, HEADS, D).transpose(0, 2, 1, 3).reshape(LOCAL, ROWS, D)


def step(queries, key_rows, value_slot_rows, out_grad, span_order):
    me = lax.axis_index("ctx")
    pos = jnp.stack([me // (Z * Y), me // Y % Z, me % Y]).astype(jnp.int32)
    kv0 = jnp.stack([key_rows.reshape(LOCAL, SPAN, D), value_slot_rows.reshape(LOCAL, SPAN, D)])
    qg0 = jnp.stack([by_head(queries), by_head(out_grad)], axis=1)
    kvz = fetch(kv0, dz=1)
    qg = [qg0, fetch(qg0, dx=1), fetch(qg0, dx=3)]
    kv = [kv0] + [fetch(kv0, dy=t) for t in range(1, Y)]
    part = stats_call(span_order, pos, qg, kv, NEAR, PLANE[:Y])
    qg += [fetch(qg[1][:1], dx=1), fetch(qg[2][1:], dx=3)]
    kv += [kvz] + [fetch(kvz, dy=t) for t in range(1, Y)]
    stats0 = stats_call(span_order, pos, qg, kv, LINE, PLANE, part)
    stats = [stats0] + [fetch(stats0, dx=t) for t in range(1, X)]
    out = grads_call(span_order, pos, qg, kv, stats)
    dq, own, other = out[:X], out[X : X + Y], out[X + Y :]

    def add(parts):
        total = parts[0].astype(jnp.float32)
        for p in parts[1:]:
            total = total + p.astype(jnp.float32)
        return total

    other = add([other[0]] + [fetch(other[t], dy=-t) for t in range(1, Y)]).astype(jnp.bfloat16)
    other = fetch(other, dz=1)
    own = add([own[0]] + [fetch(own[t], dy=-t) for t in range(1, Y)] + [other]).astype(jnp.bfloat16)
    key_gradient = own[0].reshape(LOCAL * SPAN, 1, D)
    value_gradient = own[1].reshape(LOCAL * SPAN, 1, D)
    parts = [dq[0]] + [fetch(dq[i], dx=-s) for i, s in enumerate(LINE) if i > 0]
    query_grad = (
        add(parts)
        .astype(jnp.bfloat16)
        .reshape(LOCAL, HEADS, SPAN, D)
        .transpose(0, 2, 1, 3)
        .reshape(LOCAL * SPAN, HEADS, D)
    )
    return query_grad, key_gradient, value_gradient


def solution(mesh):
    spec = P(("seq", "ctx"), "tp", None)
    return jax.shard_map(
        step,
        mesh=mesh,
        in_specs=(spec, spec, spec, spec, P("seq")),
        out_specs=(spec, spec, spec),
        check_vma=False,
    )
```
